32 devices in a mesh: ctx: 4 (over y, x), head: 8 (over z, core).
Axes of the slice: x: 2, y: 2, z: 4, core: 2. Of those that a mesh axis runs over, the one named last changes fastest.
Arguments:
- state: bfloat16 [4096, 2048], P('ctx'), may hold values from -6 to 6
- norm_gain: bfloat16 [2048], replicated, may hold values from 0.5 to 1.5
- w_qkv: bfloat16 [3, 2048, 2048], P(None, None, 'head'), may hold values from -2 to 2
- w_out: bfloat16 [2048, 2048], P('head'), may hold values from -0.125 to 0.125
- probe: bfloat16 [4096, 2048], P('ctx'), may hold values from -6 to 6
- noise: bfloat16 [4096, 2048], P(('ctx', 'head')), may hold values from -6 to 6
- segment_ids: int32 [4096], P('ctx'), may hold values from 0 to 2, never falling along the last dimension, each value on 1 to 3072 neighbouring positions
Outputs:
- new_state: float32 [4096, 2048], P(('ctx', 'head'))
The draws below stay inside these ranges and needn't reach their ends.
Inputs may be any that keep to these rules, and one draw needn't show every extreme that they name: `segment_ids`: segment numbers never fall along the sequence; a segment holds at most 3072 positions.
All inputs are finite; a program needn't handle non-finite values.
Results may differ from the reference program's by a relative error of at most 0.011.
Values may be sent and summed in bfloat16 or wider, within the bound.
A program may use at most 128 MiB of HBM per device.

```python
import math
import jax
import jax.numpy as jnp
import numpy as np
from jax import lax

D = 2048
HEADS = 16
HEAD_DIM = 128
SEQ = 4096
SEG_MOST = 3072


def state_values(key):
    noise_key = jax.random.fold_in(key, 0)
    drawn_draw = jnp.clip(jax.random.normal(noise_key, (SEQ, D), jnp.float32), -6.0, 6.0)
    result = drawn_draw
    return result


def draw_state(key, part):
    return state_values(key).astype(jnp.bfloat16)


def draw_probe(key, part):
    shared = state_values(key)
    fresh = jnp.clip(jax.random.normal(jax.random.fold_in(key, 4242), (SEQ, D), jnp.float32), -6.0, 6.0)
    return jnp.clip(0.8 * shared + 0.6 * fresh, -6.0, 6.0).astype(jnp.bfloat16)


def draw_w_qkv(key, part):
    base_key, scale_key = jax.random.split(key, 2)
    spread = D ** (-0.5)
    base_draw = jnp.clip(jax.random.normal(base_key, (3, D, D), jnp.float32), -6.0, 6.0) * spread
    head_scale = jnp.exp(jax.random.uniform(scale_key, (HEADS,), jnp.float32, jnp.log(1.2), jnp.log(1.9)))
    column_scale = jnp.repeat(head_scale, HEAD_DIM)[None, :]
    query_part = base_draw[0] * column_scale
    key_part = base_draw[1] * column_scale
    value_part = base_draw[2]
    mixed_draw = jnp.stack([query_part, key_part, value_part])
    return jnp.clip(mixed_draw, -2.0, 2.0).astype(jnp.bfloat16)


def levels(key, extent, pieces, low, top_value):
    def one(axis_at, blocks):
        heights = jax.random.uniform(jax.random.fold_in(jax.random.fold_in(key, 6), axis_at), (blocks,), jnp.float32, low / len(pieces), top_value / len(pieces))
        return jnp.repeat(jnp.exp(heights), extent[axis_at] // blocks).reshape((-1,) + (1,) * (len(extent) - axis_at - 1))

    level = one(*pieces[0])
    for cut in pieces[1:]:
        level = level * one(*cut)
    return level


def length_profile(amount, total, bound, slope):
    portions = [(1 << 20) // math.isqrt(standing ** slope) + 1 for standing in range(2, amount + 1)]
    rest, counts = total - bound - (amount - 1), [1] * (amount - 1)
    while rest > 0:
        movable = [i for i in range(amount - 1) if counts[i] < bound]
        pool, budget = sum([portions[i] for i in movable]), rest
        for i in movable:
            addition = min(bound - counts[i], max(1, budget * portions[i] // pool), rest)
            counts[i] = counts[i] + addition
            rest = rest - addition
    return np.array([bound] + counts)


def ragged_sizes(stream_key, amount, total, limit, skew):
    if amount == 2:
        one = jax.random.randint(stream_key, (), max(1, total - limit), min(limit, total - 1) + 1)
        return jnp.stack([one, total - one])
    sizes = jnp.asarray(length_profile(amount, total, limit, skew), jnp.int32)
    couples = (amount - 1) // 2
    donor, taker = sizes[1:1 + 2 * couples:2], sizes[2:2 + 2 * couples:2]
    room = jnp.minimum(donor - 1, limit - taker)
    moved = jax.random.randint(jax.random.fold_in(stream_key, 1), (couples,), 0, 1 << 20) % (room + 1)
    sizes = sizes.at[1:1 + 2 * couples:2].set(donor - moved).at[2:2 + 2 * couples:2].set(taker + moved)
    return sizes[jax.random.permutation(jax.random.fold_in(stream_key, 2), amount)]


def bell_draw(key, shape, scale, reach, pieces=(), kind=jnp.bfloat16):
    gain = levels(key, shape, pieces, -0.22, 0.18) if pieces else 1.0
    values = jax.random.normal(key, shape, jnp.float32) * scale * gain
    return jnp.minimum(jnp.maximum(values, -reach), reach).astype(kind)


def setup_inputs(seed: int = 0) -> dict:
    key_list = jax.random.split(jax.random.key(seed), 8)
    state = draw_state(jax.random.fold_in(key_list[7], 71), 0)
    norm_gain = jnp.clip(1.0 + 0.1 * jax.random.normal(key_list[1], (D,), jnp.float32), 0.5, 1.5).astype(jnp.bfloat16)
    w_qkv = draw_w_qkv(jax.random.fold_in(key_list[7], 71), 0)
    w_out = bell_draw(key_list[3], (D, D), D ** -0.5, 0.125, ((0, 8),))
    probe = draw_probe(jax.random.fold_in(key_list[7], 71), 0)
    noise = bell_draw(key_list[5], (SEQ, D), 1.0, 6.0, ((0, 32),))
    segment_ids = jnp.searchsorted(jnp.cumsum(ragged_sizes(key_list[6], 3, SEQ, SEG_MOST, 0)), jnp.arange(SEQ), side="right").astype(jnp.int32)
    return {"state": state, "norm_gain": norm_gain, "w_qkv": w_qkv, "w_out": w_out, "probe": probe, "noise": noise, "segment_ids": segment_ids}


EPSILON = 1e-05
STEP_SIZE = 0.25
NEGATIVE = -1e+30

def row_scale(matrix):
    return lax.rsqrt(lax.optimization_barrier(jnp.mean(matrix * matrix, axis=-1, keepdims=True)) + EPSILON)

def readout_grad(layer_out, probe_full):
    scale_y = row_scale(layer_out)
    return scale_y * probe_full - layer_out * scale_y ** 3 * lax.optimization_barrier(jnp.mean(probe_full * layer_out, axis=-1, keepdims=True))

def reference(state, norm_gain, w_qkv, w_out, probe, noise, segment_ids):
    state_f = state.astype(jnp.float32)
    gain_full = norm_gain.astype(jnp.float32)
    inverse = row_scale(state_f)
    normed = (state_f * inverse * gain_full).astype(jnp.bfloat16)
    score_scale = HEAD_DIM ** (-0.5)
    positions = jnp.arange(SEQ, dtype=jnp.int32)
    allowed = (positions[None, :] <= positions[:, None]) & (segment_ids[None, :] == segment_ids[:, None])
    head_proj = w_qkv.reshape(3, D, HEADS, HEAD_DIM).transpose(2, 0, 1, 3)
    head_out = w_out.reshape(HEADS, HEAD_DIM, D)

    def forward_head(weights):
        queries = jnp.dot(normed, weights[0], preferred_element_type=jnp.float32).astype(jnp.bfloat16)
        key_heads = jnp.dot(normed, weights[1], preferred_element_type=jnp.float32).astype(jnp.bfloat16)
        values = jnp.dot(normed, weights[2], preferred_element_type=jnp.float32).astype(jnp.bfloat16)
        scores = jnp.dot(queries, key_heads.T, preferred_element_type=jnp.float32) * score_scale
        scores = jnp.where(allowed, scores, NEGATIVE)
        row_max = lax.optimization_barrier(jnp.max(scores, axis=1))
        exp_scores = jnp.where(allowed, jnp.exp(scores - row_max[:, None]), 0.0)
        totals = lax.optimization_barrier(jnp.sum(exp_scores, axis=1))
        outputs = (jnp.dot(exp_scores.astype(jnp.bfloat16), values, preferred_element_type=jnp.float32) / totals[:, None]).astype(jnp.bfloat16)
        return (queries, key_heads, values, outputs, row_max + jnp.log(totals))
    queries, key_heads, values, outputs, log_totals = lax.map(forward_head, head_proj)
    joined = outputs.transpose(1, 0, 2).reshape(SEQ, D)
    layer_out = state_f + jnp.dot(joined, w_out, preferred_element_type=jnp.float32)
    readout = readout_grad(layer_out, probe.astype(jnp.float32))
    readout_half = readout.astype(jnp.bfloat16)

    def backward_head(running, head_item):
        weights, out_weight, query_h, key_h, value_h, output_h, log_h = head_item
        grads_out = jnp.dot(readout_half, out_weight.T, preferred_element_type=jnp.float32).astype(jnp.bfloat16)
        deltas = lax.optimization_barrier(jnp.sum(grads_out.astype(jnp.float32) * output_h.astype(jnp.float32), axis=1))
        scores = jnp.dot(query_h, key_h.T, preferred_element_type=jnp.float32) * score_scale
        probabilities = jnp.where(allowed, jnp.exp(scores - log_h[:, None]), 0.0)
        dprobs = jnp.dot(grads_out, value_h.T, preferred_element_type=jnp.float32)
        dscores = probabilities * (dprobs - deltas[:, None])
        prob_half = probabilities.astype(jnp.bfloat16)
        dscore_half = dscores.astype(jnp.bfloat16)
        value_grad = jnp.dot(prob_half.T, grads_out, preferred_element_type=jnp.float32).astype(jnp.bfloat16)
        key_grad = (jnp.dot(dscore_half.T, query_h, preferred_element_type=jnp.float32) * score_scale).astype(jnp.bfloat16)
        query_grad = (jnp.dot(dscore_half, key_h, preferred_element_type=jnp.float32) * score_scale).astype(jnp.bfloat16)
        running = running + jnp.dot(query_grad, weights[0].T, preferred_element_type=jnp.float32)
        running = running + jnp.dot(key_grad, weights[1].T, preferred_element_type=jnp.float32)
        running = running + jnp.dot(value_grad, weights[2].T, preferred_element_type=jnp.float32)
        return (running, None)
    normed_grad, _ = lax.scan(backward_head, jnp.zeros((SEQ, D), jnp.float32), (head_proj, head_out, queries, key_heads, values, outputs, log_totals))
    gain_grad = normed_grad * gain_full
    gradient = readout + inverse * gain_grad - state_f * inverse ** 3 * lax.optimization_barrier(jnp.mean(gain_grad * state_f, axis=-1, keepdims=True))
    return state_f - STEP_SIZE * gradient + jnp.sqrt(2.0 * STEP_SIZE) * noise.astype(jnp.float32)
```

```python
import functools

import jax
import jax.numpy as jnp
from jax import lax
from jax.experimental import pallas as pl
from jax.experimental.pallas import tpu as pltpu
from jax.sharding import PartitionSpec as P

HEAD_DIM = 128
EPSILON = 1e-05
STEP_SIZE = 0.25
NEGATIVE = -1e30
LOG2E = 1.4426950408889634
MESH = pl.DeviceIdType.MESH
VMEM = pl.BlockSpec(memory_space=pltpu.VMEM)
ANY = pl.BlockSpec(memory_space=pl.ANY)
NT = (((1,), (1,)), ((), ()))
TN = (((0,), (0,)), ((), ()))
FORWARD_BLOCKS = (256, 512)
BACKWARD_BLOCKS = (256, 512)


def row_scale(matrix):
    return lax.rsqrt(jnp.mean(matrix * matrix, axis=-1, keepdims=True) + EPSILON)


def dot32(left, right, dims):
    return lax.dot_general(left, right, dims, preferred_element_type=jnp.float32)


def greet(axis, number, me):
    barrier = pltpu.get_barrier_semaphore()
    for step in range(1, number):
        pl.semaphore_signal(
            barrier, inc=1, device_id={axis: lax.rem(me + step, number)}, device_id_type=MESH
        )
    pl.semaphore_wait(barrier, number - 1)


def gather_kernel(
    number, key_ref, value_ref, seg_ref, keys, values, segs, send_sem, recv_sem, own_sem
):
    me = lax.axis_index("ctx")
    rows = key_ref.shape[0]
    greet("ctx", number, me)
    mine = pl.ds(pl.multiple_of(me * rows, rows), rows)
    pairs = (
        (key_ref, keys.at[mine]),
        (value_ref, values.at[mine]),
        (seg_ref, segs.at[me]),
    )
    copies = []
    for step in range(1, number):
        for index, (source, target) in enumerate(pairs):
            copy = pltpu.make_async_remote_copy(
                src_ref=source,
                dst_ref=target,
                send_sem=send_sem.at[step, index],
                recv_sem=recv_sem.at[step, index],
                device_id={"ctx": lax.rem(me + step, number)},
                device_id_type=MESH,
            )
            copy.start()
            copies.append(copy)
    for index, (source, target) in enumerate(pairs):
        copy = pltpu.make_async_copy(source, target, own_sem.at[index])
        copy.start()
        copies.append(copy)
    for copy in copies:
        copy.wait()


def gather_keys(number, key_rows, value_rows, segment_ids):
    rows, width = key_rows.shape
    seg = segment_ids.reshape(-1, 128)
    full = jax.ShapeDtypeStruct((number * rows, width), key_rows.dtype)
    keys, values, segs = pl.pallas_call(
        functools.partial(gather_kernel, number),
        out_shape=(full, full, jax.ShapeDtypeStruct((number,) + seg.shape, seg.dtype)),
        in_specs=[VMEM] * 3,
        out_specs=(ANY,) * 3,
        scratch_shapes=[
            pltpu.SemaphoreType.DMA((number, 3)),
            pltpu.SemaphoreType.DMA((number, 3)),
            pltpu.SemaphoreType.DMA((3,)),
        ],
        compiler_params=pltpu.CompilerParams(collective_id=0, has_side_effects=True),
    )(key_rows, value_rows, seg)
    return keys, values, segs.reshape(-1)


def block_ranges(table, index):
    return [table[index, column] for column in range(4)]


def forward_kernel(
    heads, bq, bk, table, query_ref, key_ref, value_ref, start_ref, pos_ref, out_ref, log_ref
):
    factor = HEAD_DIM ** (-0.5) * LOG2E
    blocks = query_ref.shape[0] // bq

    def one_block(index, _):
        low, inner_low, inner_high, high = block_ranges(table, index)
        rows = pl.ds(pl.multiple_of(index * bq, bq), bq)
        start, pos = start_ref[index], pos_ref[index]

        def step(masked, piece, carry):
            keys_at = pl.ds(pl.multiple_of(piece * bk, bk), bk)
            if masked:
                key_pos = piece * bk + lax.broadcasted_iota(jnp.int32, (bk, bq), 0)
                allowed = (key_pos >= start) & (key_pos <= pos)
            result = []
            for head in range(heads):
                top, total, acc = carry[head]
                cols = pl.ds(head * HEAD_DIM, HEAD_DIM)
                scores = dot32(key_ref[keys_at, cols], query_ref[rows, cols], NT)
                if masked:
                    scores = jnp.where(allowed, scores, NEGATIVE)
                new_top = jnp.maximum(top, jnp.max(scores, axis=0, keepdims=True) * factor)
                weights = jnp.exp2(scores * factor - new_top)
                scale = jnp.exp2(top - new_top)
                total = total * scale + jnp.sum(weights, axis=0, keepdims=True)
                acc = acc * scale + dot32(
                    value_ref[keys_at, cols], weights.astype(jnp.bfloat16), TN
                )
                result.append((new_top, total, acc))
            return tuple(result)

        carry = tuple(
            (
                jnp.full((1, bq), NEGATIVE, jnp.float32),
                jnp.zeros((1, bq), jnp.float32),
                jnp.zeros((HEAD_DIM, bq), jnp.float32),
            )
            for _ in range(heads)
        )
        carry = lax.fori_loop(low, inner_low, functools.partial(step, True), carry)
        carry = lax.fori_loop(inner_low, inner_high, functools.partial(step, False), carry)
        carry = lax.fori_loop(inner_high, high, functools.partial(step, True), carry)
        for head in range(heads):
            top, total, acc = carry[head]
            out_ref[rows, pl.ds(head * HEAD_DIM, HEAD_DIM)] = (acc / total).T.astype(jnp.bfloat16)
            log_ref[index, pl.ds(head, 1), :] = top + jnp.log2(total)
        return 0

    lax.fori_loop(0, blocks, one_block, 0)


def backward_kernel(
    heads, bq, bk, table, query_ref, key_ref, value_ref, grad_ref, out_ref, log_ref, start_ref,
    pos_ref, query_out, pair_out, pair_acc,
):
    score_scale = HEAD_DIM ** (-0.5)
    factor = score_scale * LOG2E
    blocks = query_ref.shape[0] // bq
    width = heads * HEAD_DIM
    pair_rows = pair_acc.shape[0]

    def clear(piece, _):
        at = pl.ds(pl.multiple_of(piece * bk, bk), bk)
        pair_acc[at, :] = jnp.zeros((bk, 2 * width), jnp.float32)
        return 0

    lax.fori_loop(0, pair_rows // bk, clear, 0)

    def one_block(index, _):
        low, inner_low, inner_high, high = block_ranges(table, index)
        rows = pl.ds(pl.multiple_of(index * bq, bq), bq)
        start, pos = start_ref[index], pos_ref[index]
        deltas, logs = [], []
        for head in range(heads):
            cols = pl.ds(head * HEAD_DIM, HEAD_DIM)
            product = grad_ref[rows, cols].astype(jnp.float32) * out_ref[rows, cols].astype(
                jnp.float32
            )
            deltas.append(jnp.sum(product.T, axis=0, keepdims=True))
            logs.append(log_ref[index, pl.ds(head, 1), :])

        def step(masked, piece, carry):
            keys_at = pl.ds(pl.multiple_of(piece * bk, bk), bk)
            if masked:
                key_pos = piece * bk + lax.broadcasted_iota(jnp.int32, (bk, bq), 0)
                allowed = (key_pos >= start) & (key_pos <= pos)
            result = []
            for head in range(heads):
                cols = pl.ds(head * HEAD_DIM, HEAD_DIM)
                value_cols = pl.ds(width + head * HEAD_DIM, HEAD_DIM)
                key_block, query_block = key_ref[keys_at, cols], query_ref[rows, cols]
                grad_block = grad_ref[rows, cols]
                scores = dot32(key_block, query_block, NT)
                probabilities = jnp.exp2(scores * factor - logs[head])
                if masked:
                    probabilities = jnp.where(allowed, probabilities, 0.0)
                dprobs = dot32(value_ref[keys_at, cols], grad_block, NT)
                dscores = (probabilities * (dprobs - deltas[head])).astype(jnp.bfloat16)
                pair_acc[keys_at, value_cols] += jnp.dot(
                    probabilities.astype(jnp.bfloat16),
                    grad_block,
                    preferred_element_type=jnp.float32,
                )
                pair_acc[keys_at, cols] += jnp.dot(
                    dscores, query_block, preferred_element_type=jnp.float32
                )
                result.append(carry[head] + dot32(key_block, dscores, TN))
            return tuple(result)

        carry = tuple(jnp.zeros((HEAD_DIM, bq), jnp.float32) for _ in range(heads))
        carry = lax.fori_loop(low, inner_low, functools.partial(step, True), carry)
        carry = lax.fori_loop(inner_low, inner_high, functools.partial(step, False), carry)
        carry = lax.fori_loop(inner_high, high, functools.partial(step, True), carry)
        for head in range(heads):
            query_out[rows, pl.ds(head * HEAD_DIM, HEAD_DIM)] = (
                carry[head].T * score_scale
            ).astype(jnp.bfloat16)
        return 0

    lax.fori_loop(0, blocks, one_block, 0)

    def flush(piece, _):
        at = pl.ds(pl.multiple_of(piece * bk, bk), bk)
        pair_out[at, :width] = (pair_acc[at, :width] * score_scale).astype(jnp.bfloat16)
        pair_out[at, width:] = pair_acc[at, width:].astype(jnp.bfloat16)
        return 0

    lax.fori_loop(0, pair_rows // bk, flush, 0)


def make_table(start, pos, bq, bk):
    starts, places = start.reshape(-1, bq), pos.reshape(-1, bq)
    low = starts[:, 0] // bk
    inner_low = (starts[:, -1] + bk - 1) // bk
    inner_high = jnp.maximum(inner_low, (places[:, 0] + 1) // bk)
    high = places[:, -1] // bk + 1
    return jnp.stack([low, inner_low, inner_high, high], axis=1).astype(jnp.int32)


def middle_kernel(
    number, part_ref, w_any, state_ref, probe_ref, grad_out, readout_out, w_ref, joined, half,
    sending, landing, send_sem, recv_sem, back_send, back_recv, w_sem,
):
    me = lax.axis_index("head")
    width = part_ref.shape[1]
    own = state_ref.shape[0]
    model = state_ref.shape[1]
    w_copy = pltpu.make_async_copy(w_any, w_ref, w_sem)
    w_copy.start()
    greet("head", number, me)
    my_cols = pl.ds(pl.multiple_of(me * width, width), width)
    my_rows = pl.ds(pl.multiple_of(me * own, own), own)
    copies = []
    for step in range(1, number):
        peer = lax.rem(me + step, number)
        copy = pltpu.make_async_remote_copy(
            src_ref=part_ref.at[pl.ds(pl.multiple_of(peer * own, own), own)],
            dst_ref=joined.at[:, my_cols],
            send_sem=send_sem.at[step],
            recv_sem=recv_sem.at[step],
            device_id={"head": peer},
            device_id_type=MESH,
        )
        copy.start()
        copies.append(copy)
    joined[:, my_cols] = part_ref[my_rows, :]
    w_copy.wait()
    for copy in copies:
        copy.wait()

    tile = min(256, model)

    def project(piece, carry):
        squares, products = carry
        cols = pl.ds(pl.multiple_of(piece * tile, tile), tile)
        layer = state_ref[:, cols].astype(jnp.float32) + jnp.dot(
            joined[...], w_ref[:, cols], preferred_element_type=jnp.float32
        )
        readout_out[:, cols] = layer
        squares = squares + jnp.sum(layer * layer, axis=1, keepdims=True)
        products = products + jnp.sum(
            layer * probe_ref[:, cols].astype(jnp.float32), axis=1, keepdims=True
        )
        return squares, products

    zero = jnp.zeros((own, 1), jnp.float32)
    squares, products = lax.fori_loop(0, model // tile, project, (zero, zero))
    scale = lax.rsqrt(squares / model + EPSILON)
    bend = scale**3 * (products / model)

    def finish(piece, _):
        cols = pl.ds(pl.multiple_of(piece * tile, tile), tile)
        readout = scale * probe_ref[:, cols].astype(jnp.float32) - readout_out[:, cols] * bend
        readout_out[:, cols] = readout
        half[:, cols] = readout.astype(jnp.bfloat16)
        return 0

    lax.fori_loop(0, model // tile, finish, 0)
    copies = []
    for step in range(1, number):
        peer = lax.rem(me + step, number)
        sending[step] = dot32(
            half[...], w_ref[pl.ds(pl.multiple_of(peer * width, width), width), :], NT
        ).astype(jnp.bfloat16)
        copy = pltpu.make_async_remote_copy(
            src_ref=sending.at[step],
            dst_ref=landing.at[my_rows],
            send_sem=back_send.at[step],
            recv_sem=back_recv.at[step],
            device_id={"head": peer},
            device_id_type=MESH,
        )
        copy.start()
        copies.append(copy)
    landing[my_rows, :] = dot32(half[...], w_ref[my_cols, :], NT).astype(jnp.bfloat16)
    for copy in copies:
        copy.wait()
    grad_out[...] = landing[...]


def middle(number, part, w_full, state_own, probe_own):
    rows, width = part.shape
    own, model = state_own.shape
    return pl.pallas_call(
        functools.partial(middle_kernel, number),
        out_shape=(
            jax.ShapeDtypeStruct((rows, width), jnp.bfloat16),
            jax.ShapeDtypeStruct((own, model), jnp.float32),
        ),
        in_specs=[VMEM, ANY, VMEM, VMEM],
        out_specs=(VMEM, VMEM),
        scratch_shapes=[
            pltpu.VMEM(w_full.shape, jnp.bfloat16),
            pltpu.VMEM((own, number * width), jnp.bfloat16),
            pltpu.VMEM((own, model), jnp.bfloat16),
            pltpu.VMEM((number, own, width), jnp.bfloat16),
            pltpu.VMEM((rows, width), jnp.bfloat16),
            pltpu.SemaphoreType.DMA((number,)),
            pltpu.SemaphoreType.DMA((number,)),
            pltpu.SemaphoreType.DMA((number,)),
            pltpu.SemaphoreType.DMA((number,)),
            pltpu.SemaphoreType.DMA,
        ],
        compiler_params=pltpu.CompilerParams(
            collective_id=1, has_side_effects=True, vmem_limit_bytes=60 * 2**20
        ),
    )(part, w_full, state_own, probe_own)


def tail_kernel(
    ctx_count, number, pair_any, query_ref, w_ref, sum_out, own_pair, arriving, gathered, terms,
    from_partner, reduced, landing, ctx_send, ctx_recv, p_send, p_recv, z_send, z_recv, own_sem,
):
    ctx, me = lax.axis_index("ctx"), lax.axis_index("head")
    groups = number // 2
    group, core = me // 2, lax.rem(me, 2)
    partner = group * 2 + 1 - core
    rows, width = query_ref.shape
    own, model = sum_out.shape
    chunk = 2 * own
    own_copy = pltpu.make_async_copy(
        pair_any.at[pl.ds(pl.multiple_of(ctx * rows, rows), rows)], own_pair, own_sem
    )
    own_copy.start()
    barrier = pltpu.get_barrier_semaphore()
    peers = [{"ctx": lax.rem(ctx + step, ctx_count)} for step in range(1, ctx_count)]
    peers.append({"head": partner})
    for step in range(1, groups):
        peers.append({"head": lax.rem(group + step, groups) * 2 + core})
    for peer in peers:
        pl.semaphore_signal(barrier, inc=1, device_id=peer, device_id_type=MESH)
    pl.semaphore_wait(barrier, len(peers))

    def chunk_start(order):
        dest = lax.rem(group + order + 1, groups)
        return dest, pl.multiple_of(dest * chunk, chunk)

    def ctx_copy(order, step):
        target = lax.rem(ctx - step + ctx_count, ctx_count)
        _, first = chunk_start(order)
        return pltpu.make_async_remote_copy(
            src_ref=pair_any.at[pl.ds(pl.multiple_of(target * rows + first, chunk), chunk)],
            dst_ref=arriving.at[order, step - 1],
            send_sem=ctx_send.at[order, step],
            recv_sem=ctx_recv.at[order, step],
            device_id={"ctx": target},
            device_id_type=MESH,
        )

    for order in range(groups):
        for step in range(1, ctx_count):

            @pl.when(step <= ctx)
            def _():
                ctx_copy(order, step).start()

    own_copy.wait()
    tile = min(512, model)
    mine = pl.ds(pl.multiple_of(core * own, own), own)
    theirs = pl.ds(pl.multiple_of((1 - core) * own, own), own)
    waiting = []
    for order in range(groups):
        dest, first = chunk_start(order)
        at = pl.ds(first, chunk)
        gathered[...] = own_pair[at, :].astype(jnp.float32)
        for step in range(1, ctx_count):

            @pl.when(ctx + step < ctx_count)
            def _():
                ctx_copy(order, step).wait_recv()
                gathered[...] += arriving[order, step - 1].astype(jnp.float32)

        def multiply(piece, _):
            cols = pl.ds(pl.multiple_of(piece * tile, tile), tile)
            term = dot32(query_ref[at, :], w_ref[0, cols, :], NT)
            term += dot32(gathered[:, :width].astype(jnp.bfloat16), w_ref[1, cols, :], NT)
            term += dot32(gathered[:, width:].astype(jnp.bfloat16), w_ref[2, cols, :], NT)
            terms[order, :, cols] = term.astype(jnp.bfloat16)
            return 0

        lax.fori_loop(0, model // tile, multiply, 0)
        copy = pltpu.make_async_remote_copy(
            src_ref=terms.at[order, theirs],
            dst_ref=from_partner.at[order],
            send_sem=p_send.at[order],
            recv_sem=p_recv.at[order],
            device_id={"head": partner},
            device_id_type=MESH,
        )
        copy.start()
        copy.wait()
        both = terms[order, mine, :].astype(jnp.float32) + from_partner[order].astype(jnp.float32)
        if order < groups - 1:
            reduced[order] = both.astype(jnp.bfloat16)
            copy = pltpu.make_async_remote_copy(
                src_ref=reduced.at[order],
                dst_ref=landing.at[order],
                send_sem=z_send.at[order],
                recv_sem=z_recv.at[order],
                device_id={"head": dest * 2 + core},
                device_id_type=MESH,
            )
            copy.start()
            waiting.append(copy)
        else:
            sum_out[...] = both
    for order, copy in enumerate(waiting):
        copy.wait()
        sum_out[...] += landing[order].astype(jnp.float32)
    for order in range(groups):
        for step in range(1, ctx_count):

            @pl.when(step <= ctx)
            def _():
                ctx_copy(order, step).wait_send()


def tail(ctx_count, number, pair, query_grad, w_qkv):
    rows, width = query_grad.shape
    model = w_qkv.shape[1]
    own, groups = rows // number, number // 2
    half, full = jnp.bfloat16, jnp.float32
    dma = pltpu.SemaphoreType.DMA
    return pl.pallas_call(
        functools.partial(tail_kernel, ctx_count, number),
        out_shape=jax.ShapeDtypeStruct((own, model), full),
        in_specs=[ANY, VMEM, VMEM],
        out_specs=VMEM,
        scratch_shapes=[
            pltpu.VMEM((rows, 2 * width), half),
            pltpu.VMEM((groups, ctx_count - 1, 2 * own, 2 * width), half),
            pltpu.VMEM((2 * own, 2 * width), full),
            pltpu.VMEM((groups, 2 * own, model), half),
            pltpu.VMEM((groups, own, model), half),
            pltpu.VMEM((groups, own, model), half),
            pltpu.VMEM((groups, own, model), half),
            dma((groups, ctx_count)),
            dma((groups, ctx_count)),
            dma((groups,)),
            dma((groups,)),
            dma((groups,)),
            dma((groups,)),
            dma,
        ],
        compiler_params=pltpu.CompilerParams(
            collective_id=2, has_side_effects=True, vmem_limit_bytes=60 * 2**20
        ),
    )(pair, query_grad, w_qkv)


def body(state, norm_gain, w_qkv, w_out, probe, noise, segment_ids):
    local_rows, model_width = state.shape
    width = w_qkv.shape[2]
    local_heads = width // HEAD_DIM
    head_count = lax.axis_size("head")
    ctx_count = lax.axis_size("ctx")
    ctx_index = lax.axis_index("ctx")
    own_rows = local_rows // head_count
    row_start = lax.axis_index("head") * own_rows
    w_full = lax.all_gather(w_out, "head", axis=0, tiled=True)
    state_f = state.astype(jnp.float32)
    gain_full = norm_gain.astype(jnp.float32)
    inverse = row_scale(state_f)
    normed = (state_f * inverse * gain_full).astype(jnp.bfloat16)

    def project(index):
        return jnp.dot(normed, w_qkv[index], preferred_element_type=jnp.float32).astype(
            jnp.bfloat16
        )

    query_rows, key_rows, value_rows = project(0), project(1), project(2)
    keys, values, segs = gather_keys(ctx_count, key_rows, value_rows, segment_ids)
    total_rows = keys.shape[0]
    pos = ctx_index * local_rows + jnp.arange(local_rows, dtype=jnp.int32)
    start = jnp.sum((segs[None, :] < segment_ids[:, None]).astype(jnp.int32), axis=1)
    fq, fk = (min(local_rows, size) for size in FORWARD_BLOCKS)
    gq, gk = (min(local_rows, size) for size in BACKWARD_BLOCKS)
    smem = pl.BlockSpec(memory_space=pltpu.SMEM)
    params = pltpu.CompilerParams(vmem_limit_bytes=60 * 2**20)
    outputs, logs = pl.pallas_call(
        functools.partial(forward_kernel, local_heads, fq, fk),
        out_shape=(
            jax.ShapeDtypeStruct((local_rows, width), jnp.bfloat16),
            jax.ShapeDtypeStruct((local_rows // fq, local_heads, fq), jnp.float32),
        ),
        in_specs=[smem] + [VMEM] * 5,
        out_specs=(VMEM, VMEM),
        compiler_params=params,
        cost_estimate=pl.CostEstimate(
            flops=4 * local_rows * total_rows * width, bytes_accessed=0, transcendentals=0
        ),
    )(
        make_table(start, pos, fq, fk),
        query_rows,
        keys,
        values,
        start.reshape(-1, 1, fq),
        pos.reshape(-1, 1, fq),
    )
    state_half = lax.dynamic_slice_in_dim(state, row_start, own_rows, 0)
    probe_own = lax.dynamic_slice_in_dim(probe, row_start, own_rows, 0)
    state_own = state_half.astype(jnp.float32)
    inverse_own = row_scale(state_own)
    grads_out, readout_own = middle(head_count, outputs, w_full, state_half, probe_own)
    query_grad, pair = pl.pallas_call(
        functools.partial(backward_kernel, local_heads, gq, gk),
        out_shape=(
            jax.ShapeDtypeStruct((local_rows, width), jnp.bfloat16),
            jax.ShapeDtypeStruct((total_rows, 2 * width), jnp.bfloat16),
        ),
        in_specs=[smem] + [VMEM] * 8,
        out_specs=(VMEM, VMEM),
        scratch_shapes=[pltpu.VMEM((total_rows, 2 * width), jnp.float32)],
        compiler_params=params,
        cost_estimate=pl.CostEstimate(
            flops=10 * local_rows * total_rows * width, bytes_accessed=0, transcendentals=0
        ),
    )(
        make_table(start, pos, gq, gk),
        query_rows,
        keys,
        values,
        grads_out,
        outputs,
        logs.reshape(local_rows // fq, local_heads, fq),
        start.reshape(-1, 1, gq),
        pos.reshape(-1, 1, gq),
    )
    normed_grad = tail(ctx_count, head_count, pair, query_grad, w_qkv)
    gain_grad = normed_grad * gain_full
    gradient = (
        readout_own
        + inverse_own * gain_grad
        - state_own * inverse_own**3 * jnp.mean(gain_grad * state_own, axis=-1, keepdims=True)
    )
    return state_own - STEP_SIZE * gradient + jnp.sqrt(2.0 * STEP_SIZE) * noise.astype(jnp.float32)


def solution(mesh):
    placed = (
        P("ctx", None),
        P(),
        P(None, None, "head"),
        P("head", None),
        P("ctx", None),
        P(("ctx", "head"), None),
        P("ctx"),
    )
    return jax.shard_map(
        body, mesh=mesh, in_specs=placed, out_specs=P(("ctx", "head"), None), check_vma=False
    )
```

```python
import functools

import jax
import jax.numpy as jnp
from jax import lax
from jax.experimental import pallas as pl
from jax.experimental.pallas import tpu as pltpu
from jax.sharding import PartitionSpec as P

HEAD_DIM = 128
EPSILON = 1e-05
STEP_SIZE = 0.25
NEGATIVE = -1e30
LOG2E = 1.4426950408889634
MESH = pl.DeviceIdType.MESH
VMEM = pl.BlockSpec(memory_space=pltpu.VMEM)
ANY = pl.BlockSpec(memory_space=pl.ANY)
NT = (((1,), (1,)), ((), ()))
TN = (((0,), (0,)), ((), ()))
FORWARD_BLOCKS = (512, 512)
BACKWARD_BLOCKS = (512, 512)


def row_scale(matrix):
    return lax.rsqrt(jnp.mean(matrix * matrix, axis=-1, keepdims=True) + EPSILON)


def dot32(left, right, dims):
    return lax.dot_general(left, right, dims, preferred_element_type=jnp.float32)


def greet(axis, number, me):
    barrier = pltpu.get_barrier_semaphore()
    for step in range(1, number):
        pl.semaphore_signal(
            barrier, inc=1, device_id={axis: lax.rem(me + step, number)}, device_id_type=MESH
        )
    pl.semaphore_wait(barrier, number - 1)


def gather_kernel(
    number, key_ref, value_ref, seg_ref, normed_ref, w_ref, keys, values, segs, query_out, send_sem,
    recv_sem, own_sem,
):
    me = lax.axis_index("ctx")
    rows = key_ref.shape[0]
    greet("ctx", number, me)

    def place(index):
        return pl.ds(pl.multiple_of(index * rows, rows), rows)

    def send(slot, source, target, peer):
        copy = pltpu.make_async_remote_copy(
            src_ref=source,
            dst_ref=target,
            send_sem=send_sem.at[slot],
            recv_sem=recv_sem.at[slot],
            device_id={"ctx": peer},
            device_id_type=MESH,
        )
        copy.start()
        return copy

    mine = place(me)
    copies = []
    for step in range(1, number):
        copies.append(send(step, seg_ref, segs.at[me], lax.rem(me + step, number)))
    relay = number == 4
    if relay:
        low, high = lax.rem(me, 2), me // 2
        across, along = high * 2 + 1 - low, (1 - high) * 2 + low
        key_first = send(number, key_ref, keys.at[mine], across)
        value_first = send(number + 1, value_ref, values.at[mine], along)
        copies.append(send(number + 2, value_ref, values.at[mine], across))
        copies.append(send(number + 3, key_ref, keys.at[mine], along))
    else:
        for step in range(1, number):
            peer = lax.rem(me + step, number)
            copies.append(send(number + 2 * step, key_ref, keys.at[mine], peer))
            copies.append(send(number + 2 * step + 1, value_ref, values.at[mine], peer))
    pairs = ((key_ref, keys.at[mine]), (value_ref, values.at[mine]), (seg_ref, segs.at[me]))
    for index, (source, target) in enumerate(pairs):
        copy = pltpu.make_async_copy(source, target, own_sem.at[index])
        copy.start()
        copies.append(copy)
    tile = min(256, rows)

    def project(piece, _):
        at = pl.ds(pl.multiple_of(piece * tile, tile), tile)
        query_out[at, :] = jnp.dot(
            normed_ref[at, :], w_ref[...], preferred_element_type=jnp.float32
        ).astype(jnp.bfloat16)
        return 0

    lax.fori_loop(0, rows // tile, project, 0)
    if relay:
        key_first.wait()
        copies.append(send(number + 4, keys.at[place(across)], keys.at[place(across)], along))
        value_first.wait()
        copies.append(send(number + 5, values.at[place(along)], values.at[place(along)], across))
    for copy in copies:
        copy.wait()


def gather_keys(number, key_rows, value_rows, segment_ids, normed, w_query):
    rows, width = key_rows.shape
    seg = segment_ids.reshape(-1, 128)
    full = jax.ShapeDtypeStruct((number * rows, width), key_rows.dtype)
    keys, values, segs, queries = pl.pallas_call(
        functools.partial(gather_kernel, number),
        out_shape=(
            full,
            full,
            jax.ShapeDtypeStruct((number,) + seg.shape, seg.dtype),
            jax.ShapeDtypeStruct((rows, width), key_rows.dtype),
        ),
        in_specs=[VMEM] * 5,
        out_specs=(ANY, ANY, ANY, VMEM),
        scratch_shapes=[
            pltpu.SemaphoreType.DMA((3 * number + 6,)),
            pltpu.SemaphoreType.DMA((3 * number + 6,)),
            pltpu.SemaphoreType.DMA((3,)),
        ],
        compiler_params=pltpu.CompilerParams(collective_id=0, has_side_effects=True),
    )(key_rows, value_rows, seg, normed, w_query)
    return keys, values, segs.reshape(-1), queries


def block_ranges(table, index):
    return [table[index, column] for column in range(4)]


def forward_kernel(
    heads, bq, bk, table, query_ref, key_ref, value_ref, start_ref, pos_ref, out_ref, log_ref
):
    factor = HEAD_DIM ** (-0.5) * LOG2E
    blocks = query_ref.shape[0] // bq

    def one_block(index, _):
        low, inner_low, inner_high, high = block_ranges(table, index)
        rows = pl.ds(pl.multiple_of(index * bq, bq), bq)
        start, pos = start_ref[index], pos_ref[index]

        def step(masked, piece, carry):
            keys_at = pl.ds(pl.multiple_of(piece * bk, bk), bk)
            if masked:
                key_pos = piece * bk + lax.broadcasted_iota(jnp.int32, (bk, bq), 0)
                allowed = (key_pos >= start) & (key_pos <= pos)
            result = []
            for head in range(heads):
                top, total, acc = carry[head]
                cols = pl.ds(head * HEAD_DIM, HEAD_DIM)
                scores = dot32(key_ref[keys_at, cols], query_ref[rows, cols], NT)
                if masked:
                    scores = jnp.where(allowed, scores, NEGATIVE)
                new_top = jnp.maximum(top, jnp.max(scores, axis=0, keepdims=True) * factor)
                weights = jnp.exp2(scores * factor - new_top)
                scale = jnp.exp2(top - new_top)
                total = total * scale + jnp.sum(weights, axis=0, keepdims=True)
                acc = acc * scale + dot32(
                    value_ref[keys_at, cols], weights.astype(jnp.bfloat16), TN
                )
                result.append((new_top, total, acc))
            return tuple(result)

        carry = tuple(
            (
                jnp.full((1, bq), NEGATIVE, jnp.float32),
                jnp.zeros((1, bq), jnp.float32),
                jnp.zeros((HEAD_DIM, bq), jnp.float32),
            )
            for _ in range(heads)
        )
        carry = lax.fori_loop(low, inner_low, functools.partial(step, True), carry)
        carry = lax.fori_loop(inner_low, inner_high, functools.partial(step, False), carry)
        carry = lax.fori_loop(inner_high, high, functools.partial(step, True), carry)
        for head in range(heads):
            top, total, acc = carry[head]
            out_ref[rows, pl.ds(head * HEAD_DIM, HEAD_DIM)] = (acc / total).T.astype(jnp.bfloat16)
            log_ref[index, pl.ds(head, 1), :] = top + jnp.log2(total)
        return 0

    lax.fori_loop(0, blocks, one_block, 0)


def backward_kernel(
    heads, bq, bk, table, query_ref, key_ref, value_ref, grad_ref, out_ref, log_ref, start_ref,
    pos_ref, query_out, pair_out, pair_acc,
):
    score_scale = HEAD_DIM ** (-0.5)
    factor = score_scale * LOG2E
    blocks = query_ref.shape[0] // bq
    width = heads * HEAD_DIM
    pair_rows = pair_acc.shape[0]

    def clear(piece, _):
        at = pl.ds(pl.multiple_of(piece * bk, bk), bk)
        pair_acc[at, :] = jnp.zeros((bk, 2 * width), jnp.float32)
        return 0

    lax.fori_loop(0, pair_rows // bk, clear, 0)

    def one_block(index, _):
        low, inner_low, inner_high, high = block_ranges(table, index)
        rows = pl.ds(pl.multiple_of(index * bq, bq), bq)
        start, pos = start_ref[index], pos_ref[index]
        deltas, logs = [], []
        for head in range(heads):
            cols = pl.ds(head * HEAD_DIM, HEAD_DIM)
            product = grad_ref[rows, cols].astype(jnp.float32) * out_ref[rows, cols].astype(
                jnp.float32
            )
            deltas.append(jnp.sum(product.T, axis=0, keepdims=True))
            logs.append(log_ref[index, pl.ds(head, 1), :])

        def step(masked, piece, carry):
            keys_at = pl.ds(pl.multiple_of(piece * bk, bk), bk)
            if masked:
                key_pos = piece * bk + lax.broadcasted_iota(jnp.int32, (bk, bq), 0)
                allowed = (key_pos >= start) & (key_pos <= pos)
            result = []
            for head in range(heads):
                cols = pl.ds(head * HEAD_DIM, HEAD_DIM)
                value_cols = pl.ds(width + head * HEAD_DIM, HEAD_DIM)
                key_block, query_block = key_ref[keys_at, cols], query_ref[rows, cols]
                grad_block = grad_ref[rows, cols]
                scores = dot32(key_block, query_block, NT)
                probabilities = jnp.exp2(scores * factor - logs[head])
                if masked:
                    probabilities = jnp.where(allowed, probabilities, 0.0)
                dprobs = dot32(value_ref[keys_at, cols], grad_block, NT)
                dscores = (probabilities * (dprobs - deltas[head])).astype(jnp.bfloat16)
                pair_acc[keys_at, value_cols] += jnp.dot(
                    probabilities.astype(jnp.bfloat16),
                    grad_block,
                    preferred_element_type=jnp.float32,
                )
                pair_acc[keys_at, cols] += jnp.dot(
                    dscores, query_block, preferred_element_type=jnp.float32
                )
                result.append(carry[head] + dot32(key_block, dscores, TN))
            return tuple(result)

        carry = tuple(jnp.zeros((HEAD_DIM, bq), jnp.float32) for _ in range(heads))
        carry = lax.fori_loop(low, inner_low, functools.partial(step, True), carry)
        carry = lax.fori_loop(inner_low, inner_high, functools.partial(step, False), carry)
        carry = lax.fori_loop(inner_high, high, functools.partial(step, True), carry)
        for head in range(heads):
            query_out[rows, pl.ds(head * HEAD_DIM, HEAD_DIM)] = (
                carry[head].T * score_scale
            ).astype(jnp.bfloat16)
        return 0

    lax.fori_loop(0, blocks, one_block, 0)

    def flush(piece, _):
        at = pl.ds(pl.multiple_of(piece * bk, bk), bk)
        pair_out[at, :width] = (pair_acc[at, :width] * score_scale).astype(jnp.bfloat16)
        pair_out[at, width:] = pair_acc[at, width:].astype(jnp.bfloat16)
        return 0

    lax.fori_loop(0, pair_rows // bk, flush, 0)


def make_table(start, pos, bq, bk):
    starts, places = start.reshape(-1, bq), pos.reshape(-1, bq)
    low = starts[:, 0] // bk
    inner_low = (starts[:, -1] + bk - 1) // bk
    inner_high = jnp.maximum(inner_low, (places[:, 0] + 1) // bk)
    high = places[:, -1] // bk + 1
    return jnp.stack([low, inner_low, inner_high, high], axis=1).astype(jnp.int32)


def middle_kernel(
    number, part_ref, w_any, state_ref, probe_ref, grad_out, readout_out, w_ref, joined, half,
    sending, landing, send_sem, recv_sem, back_send, back_recv, w_sem,
):
    me = lax.axis_index("head")
    width = part_ref.shape[1]
    own = state_ref.shape[0]
    model = state_ref.shape[1]
    w_copy = pltpu.make_async_copy(w_any, w_ref, w_sem)
    w_copy.start()
    greet("head", number, me)
    my_cols = pl.ds(pl.multiple_of(me * width, width), width)
    my_rows = pl.ds(pl.multiple_of(me * own, own), own)
    copies = []
    for step in range(1, number):
        peer = lax.rem(me + step, number)
        copy = pltpu.make_async_remote_copy(
            src_ref=part_ref.at[pl.ds(pl.multiple_of(peer * own, own), own)],
            dst_ref=joined.at[:, my_cols],
            send_sem=send_sem.at[step],
            recv_sem=recv_sem.at[step],
            device_id={"head": peer},
            device_id_type=MESH,
        )
        copy.start()
        copies.append(copy)
    joined[:, my_cols] = part_ref[my_rows, :]
    w_copy.wait()
    for copy in copies:
        copy.wait()

    tile = min(256, model)

    def project(piece, carry):
        squares, products = carry
        cols = pl.ds(pl.multiple_of(piece * tile, tile), tile)
        layer = state_ref[:, cols].astype(jnp.float32) + jnp.dot(
            joined[...], w_ref[:, cols], preferred_element_type=jnp.float32
        )
        readout_out[:, cols] = layer
        squares = squares + jnp.sum(layer * layer, axis=1, keepdims=True)
        products = products + jnp.sum(
            layer * probe_ref[:, cols].astype(jnp.float32), axis=1, keepdims=True
        )
        return squares, products

    zero = jnp.zeros((own, 1), jnp.float32)
    squares, products = lax.fori_loop(0, model // tile, project, (zero, zero))
    scale = lax.rsqrt(squares / model + EPSILON)
    bend = scale**3 * (products / model)

    def finish(piece, _):
        cols = pl.ds(pl.multiple_of(piece * tile, tile), tile)
        readout = scale * probe_ref[:, cols].astype(jnp.float32) - readout_out[:, cols] * bend
        readout_out[:, cols] = readout
        half[:, cols] = readout.astype(jnp.bfloat16)
        return 0

    lax.fori_loop(0, model // tile, finish, 0)
    copies = []
    for step in range(1, number):
        peer = lax.rem(me + step, number)
        sending[step] = dot32(
            half[...], w_ref[pl.ds(pl.multiple_of(peer * width, width), width), :], NT
        ).astype(jnp.bfloat16)
        copy = pltpu.make_async_remote_copy(
            src_ref=sending.at[step],
            dst_ref=landing.at[my_rows],
            send_sem=back_send.at[step],
            recv_sem=back_recv.at[step],
            device_id={"head": peer},
            device_id_type=MESH,
        )
        copy.start()
        copies.append(copy)
    landing[my_rows, :] = dot32(half[...], w_ref[my_cols, :], NT).astype(jnp.bfloat16)
    for copy in copies:
        copy.wait()
    grad_out[...] = landing[...]


def middle(number, part, w_full, state_own, probe_own):
    rows, width = part.shape
    own, model = state_own.shape
    return pl.pallas_call(
        functools.partial(middle_kernel, number),
        out_shape=(
            jax.ShapeDtypeStruct((rows, width), jnp.bfloat16),
            jax.ShapeDtypeStruct((own, model), jnp.float32),
        ),
        in_specs=[VMEM, ANY, VMEM, VMEM],
        out_specs=(VMEM, VMEM),
        scratch_shapes=[
            pltpu.VMEM(w_full.shape, jnp.bfloat16),
            pltpu.VMEM((own, number * width), jnp.bfloat16),
            pltpu.VMEM((own, model), jnp.bfloat16),
            pltpu.VMEM((number, own, width), jnp.bfloat16),
            pltpu.VMEM((rows, width), jnp.bfloat16),
            pltpu.SemaphoreType.DMA((number,)),
            pltpu.SemaphoreType.DMA((number,)),
            pltpu.SemaphoreType.DMA((number,)),
            pltpu.SemaphoreType.DMA((number,)),
            pltpu.SemaphoreType.DMA,
        ],
        compiler_params=pltpu.CompilerParams(
            collective_id=1, has_side_effects=True, vmem_limit_bytes=60 * 2**20
        ),
    )(part, w_full, state_own, probe_own)


def tail_kernel(
    ctx_count, number, pair_any, query_ref, w_ref, sum_out, own_pair, arriving, gathered, terms,
    from_partner, reduced, landing, ctx_send, ctx_recv, p_send, p_recv, z_send, z_recv, own_sem,
):
    ctx, me = lax.axis_index("ctx"), lax.axis_index("head")
    groups = number // 2
    group, core = me // 2, lax.rem(me, 2)
    partner = group * 2 + 1 - core
    rows, width = query_ref.shape
    own, model = sum_out.shape
    chunk = 2 * own
    own_copy = pltpu.make_async_copy(
        pair_any.at[pl.ds(pl.multiple_of(ctx * rows, rows), rows)], own_pair, own_sem
    )
    own_copy.start()
    barrier = pltpu.get_barrier_semaphore()
    peers = [{"ctx": lax.rem(ctx + step, ctx_count)} for step in range(1, ctx_count)]
    peers.append({"head": partner})
    for step in range(1, groups):
        peers.append({"head": lax.rem(group + step, groups) * 2 + core})
    for peer in peers:
        pl.semaphore_signal(barrier, inc=1, device_id=peer, device_id_type=MESH)
    pl.semaphore_wait(barrier, len(peers))

    def chunk_start(order):
        dest = lax.rem(group + order + 1, groups)
        return dest, pl.multiple_of(dest * chunk, chunk)

    def ctx_copy(order, step):
        target = lax.rem(ctx - step + ctx_count, ctx_count)
        _, first = chunk_start(order)
        return pltpu.make_async_remote_copy(
            src_ref=pair_any.at[pl.ds(pl.multiple_of(target * rows + first, chunk), chunk)],
            dst_ref=arriving.at[order, step - 1],
            send_sem=ctx_send.at[order, step],
            recv_sem=ctx_recv.at[order, step],
            device_id={"ctx": target},
            device_id_type=MESH,
        )

    for order in range(groups):
        for step in range(1, ctx_count):

            @pl.when(step <= ctx)
            def _():
                ctx_copy(order, step).start()

    own_copy.wait()
    tile = min(512, model)
    mine = pl.ds(pl.multiple_of(core * own, own), own)
    theirs = pl.ds(pl.multiple_of((1 - core) * own, own), own)
    waiting = []
    for order in range(groups):
        dest, first = chunk_start(order)
        at = pl.ds(first, chunk)
        gathered[...] = own_pair[at, :].astype(jnp.float32)
        for step in range(1, ctx_count):

            @pl.when(ctx + step < ctx_count)
            def _():
                ctx_copy(order, step).wait_recv()
                gathered[...] += arriving[order, step - 1].astype(jnp.float32)

        def multiply(piece, _):
            cols = pl.ds(pl.multiple_of(piece * tile, tile), tile)
            term = dot32(query_ref[at, :], w_ref[0, cols, :], NT)
            term += dot32(gathered[:, :width].astype(jnp.bfloat16), w_ref[1, cols, :], NT)
            term += dot32(gathered[:, width:].astype(jnp.bfloat16), w_ref[2, cols, :], NT)
            terms[order, :, cols] = term.astype(jnp.bfloat16)
            return 0

        lax.fori_loop(0, model // tile, multiply, 0)
        copy = pltpu.make_async_remote_copy(
            src_ref=terms.at[order, theirs],
            dst_ref=from_partner.at[order],
            send_sem=p_send.at[order],
            recv_sem=p_recv.at[order],
            device_id={"head": partner},
            device_id_type=MESH,
        )
        copy.start()
        copy.wait()
        both = terms[order, mine, :].astype(jnp.float32) + from_partner[order].astype(jnp.float32)
        if order < groups - 1:
            reduced[order] = both.astype(jnp.bfloat16)
            copy = pltpu.make_async_remote_copy(
                src_ref=reduced.at[order],
                dst_ref=landing.at[order],
                send_sem=z_send.at[order],
                recv_sem=z_recv.at[order],
                device_id={"head": dest * 2 + core},
                device_id_type=MESH,
            )
            copy.start()
            waiting.append(copy)
        else:
            sum_out[...] = both
    for order, copy in enumerate(waiting):
        copy.wait()
        sum_out[...] += landing[order].astype(jnp.float32)
    for order in range(groups):
        for step in range(1, ctx_count):

            @pl.when(step <= ctx)
            def _():
                ctx_copy(order, step).wait_send()


def tail(ctx_count, number, pair, query_grad, w_qkv):
    rows, width = query_grad.shape
    model = w_qkv.shape[1]
    own, groups = rows // number, number // 2
    half, full = jnp.bfloat16, jnp.float32
    dma = pltpu.SemaphoreType.DMA
    return pl.pallas_call(
        functools.partial(tail_kernel, ctx_count, number),
        out_shape=jax.ShapeDtypeStruct((own, model), full),
        in_specs=[ANY, VMEM, VMEM],
        out_specs=VMEM,
        scratch_shapes=[
            pltpu.VMEM((rows, 2 * width), half),
            pltpu.VMEM((groups, ctx_count - 1, 2 * own, 2 * width), half),
            pltpu.VMEM((2 * own, 2 * width), full),
            pltpu.VMEM((groups, 2 * own, model), half),
            pltpu.VMEM((groups, own, model), half),
            pltpu.VMEM((groups, own, model), half),
            pltpu.VMEM((groups, own, model), half),
            dma((groups, ctx_count)),
            dma((groups, ctx_count)),
            dma((groups,)),
            dma((groups,)),
            dma((groups,)),
            dma((groups,)),
            dma,
        ],
        compiler_params=pltpu.CompilerParams(
            collective_id=2, has_side_effects=True, vmem_limit_bytes=60 * 2**20
        ),
    )(pair, query_grad, w_qkv)


def body(state, norm_gain, w_qkv, w_out, probe, noise, segment_ids):
    local_rows, model_width = state.shape
    width = w_qkv.shape[2]
    local_heads = width // HEAD_DIM
    head_count = lax.axis_size("head")
    ctx_count = lax.axis_size("ctx")
    ctx_index = lax.axis_index("ctx")
    own_rows = local_rows // head_count
    row_start = lax.axis_index("head") * own_rows
    w_full = lax.all_gather(w_out, "head", axis=0, tiled=True)
    state_f = state.astype(jnp.float32)
    gain_full = norm_gain.astype(jnp.float32)
    inverse = row_scale(state_f)
    normed = (state_f * inverse * gain_full).astype(jnp.bfloat16)

    def project(index):
        return jnp.dot(normed, w_qkv[index], preferred_element_type=jnp.float32).astype(
            jnp.bfloat16
        )

    key_rows, value_rows = project(1), project(2)
    keys, values, segs, query_rows = gather_keys(
        ctx_count, key_rows, value_rows, segment_ids, normed, w_qkv[0]
    )
    total_rows = keys.shape[0]
    pos = ctx_index * local_rows + jnp.arange(local_rows, dtype=jnp.int32)
    start = jnp.sum((segs[None, :] < segment_ids[:, None]).astype(jnp.int32), axis=1)
    fq, fk = (min(local_rows, size) for size in FORWARD_BLOCKS)
    gq, gk = (min(local_rows, size) for size in BACKWARD_BLOCKS)
    smem = pl.BlockSpec(memory_space=pltpu.SMEM)
    params = pltpu.CompilerParams(vmem_limit_bytes=60 * 2**20)
    outputs, logs = pl.pallas_call(
        functools.partial(forward_kernel, local_heads, fq, fk),
        out_shape=(
            jax.ShapeDtypeStruct((local_rows, width), jnp.bfloat16),
            jax.ShapeDtypeStruct((local_rows // fq, local_heads, fq), jnp.float32),
        ),
        in_specs=[smem] + [VMEM] * 5,
        out_specs=(VMEM, VMEM),
        compiler_params=params,
        cost_estimate=pl.CostEstimate(
            flops=4 * local_rows * total_rows * width, bytes_accessed=0, transcendentals=0
        ),
    )(
        make_table(start, pos, fq, fk),
        query_rows,
        keys,
        values,
        start.reshape(-1, 1, fq),
        pos.reshape(-1, 1, fq),
    )
    state_half = lax.dynamic_slice_in_dim(state, row_start, own_rows, 0)
    probe_own = lax.dynamic_slice_in_dim(probe, row_start, own_rows, 0)
    state_own = state_half.astype(jnp.float32)
    inverse_own = row_scale(state_own)
    grads_out, readout_own = middle(head_count, outputs, w_full, state_half, probe_own)
    query_grad, pair = pl.pallas_call(
        functools.partial(backward_kernel, local_heads, gq, gk),
        out_shape=(
            jax.ShapeDtypeStruct((local_rows, width), jnp.bfloat16),
            jax.ShapeDtypeStruct((total_rows, 2 * width), jnp.bfloat16),
        ),
        in_specs=[smem] + [VMEM] * 8,
        out_specs=(VMEM, VMEM),
        scratch_shapes=[pltpu.VMEM((total_rows, 2 * width), jnp.float32)],
        compiler_params=params,
        cost_estimate=pl.CostEstimate(
            flops=10 * local_rows * total_rows * width, bytes_accessed=0, transcendentals=0
        ),
    )(
        make_table(start, pos, gq, gk),
        query_rows,
        keys,
        values,
        grads_out,
        outputs,
        logs.reshape(local_rows // fq, local_heads, fq),
        start.reshape(-1, 1, gq),
        pos.reshape(-1, 1, gq),
    )
    normed_grad = tail(ctx_count, head_count, pair, query_grad, w_qkv)
    gain_grad = normed_grad * gain_full
    gradient = (
        readout_own
        + inverse_own * gain_grad
        - state_own * inverse_own**3 * jnp.mean(gain_grad * state_own, axis=-1, keepdims=True)
    )
    return state_own - STEP_SIZE * gradient + jnp.sqrt(2.0 * STEP_SIZE) * noise.astype(jnp.float32)


def solution(mesh):
    placed = (
        P("ctx", None),
        P(),
        P(None, None, "head"),
        P("head", None),
        P("ctx", None),
        P(("ctx", "head"), None),
        P("ctx"),
    )
    return jax.shard_map(
        body, mesh=mesh, in_specs=placed, out_specs=P(("ctx", "head"), None), check_vma=False
    )
```
